32 devices in a mesh: batch: 8 (over z, core), seq: 4 (over y, x).
Axes of the slice: x: 2, y: 2, z: 4, core: 2. Of those that a mesh axis runs over, the one named last changes fastest.
Arguments:
- token_cond: bfloat16 [16384, 768], P(('batch', 'seq')), parts along dimension 0, may hold values from -6 to 6
- atom_feat: bfloat16 [131072, 128], P(('batch', 'seq')), parts along dimension 0, may hold values from -16 to 16
- atom_counts: int32 [16384], P(('batch', 'seq')), parts along dimension 0, may hold values from 1 to 24, as said below
- w_token: bfloat16 [768, 128], replicated, may hold values from -0.21875 to 0.21875
- w_query: bfloat16 [128, 128], replicated, may hold values from -0.5 to 0.5
- w_key: bfloat16 [128, 128], replicated, may hold values from -0.5 to 0.5
- w_value: bfloat16 [128, 128], replicated, may hold values from -0.5 to 0.5
- w_out: bfloat16 [128, 128], replicated, may hold values from -0.5 to 0.5
- w_back: bfloat16 [128, 768], replicated, may hold values from -0.5 to 0.5
Outputs:
- token_out: bfloat16 [16384, 768], P(('batch', 'seq')), parts along dimension 0
- atom_out: bfloat16 [131072, 128], P(('batch', 'seq')), parts along dimension 0
The draws below stay inside these ranges and needn't reach their ends.
There are 8 independent parts, one for each index of `batch`. The reference program is written for one: setup_inputs(seed, part) draws one part's arguments, and reference() takes and returns one part's arrays. A program takes and returns all parts, laid end to end along the dimension named above; an argument that names none is the same for every part. Nothing has to cross between parts.
Inputs may be any that keep to these rules, and one draw needn't show every extreme that they name: `atom_counts`: every token has at least one atom and the counts of one complex sum to 16384. For every k, the atoms k * 4096 to (k + 1) * 4096 - 1 belong to tokens of (k - 1) * 512 to (k + 2) * 512 - 1.
All inputs are finite; a program needn't handle non-finite values.
Results may differ from the reference program's by a relative error of at most 0.0095.
The reference program's roundings to bfloat16 on the way count: a program that leaves them out, or rounds other values in their place, can miss the bound.
Values may be sent and summed in bfloat16 or wider, within the bound.
A program may use at most 128 MiB of HBM per device.

```python
import jax
import jax.numpy as jnp

CT = 768
CA = 128
HEADS = 4
HEAD = 32
QBLOCK = 32
KEYS = 128
MOST = 24
TOK_DEV = 512
ATOM_DEV = 4096
HALO = 48
NTOK = 2048
NATOM = 16384


def draw_atom_feat(key, part):
    first = jax.random.fold_in(jax.random.fold_in(key, 11), 0)
    values = jax.random.normal(first, (NATOM, CA), jnp.float32)
    values = jnp.clip(values, -6.0, 6.0)
    return values.astype(jnp.bfloat16)


def draw_atom_counts(key, part):
    first, second, third, fourth, fifth = jax.random.split(jax.random.fold_in(key, 23), 5)
    nblocks = NTOK // TOK_DEV
    slots = MOST - 1
    magnitude = jax.random.randint(first, (nblocks - 1,), 2 * TOK_DEV, 3 * TOK_DEV + 1)
    flip = jax.random.randint(second, (), 0, 2)
    signs = 1 - 2 * ((jnp.arange(nblocks - 1, dtype=jnp.int32) + flip) % 2)
    drift = jnp.concatenate([jnp.zeros((1,), jnp.int32), (magnitude * signs).astype(jnp.int32), jnp.zeros((1,), jnp.int32)])
    block_sum = ATOM_DEV + drift[1:] - drift[:-1]
    extra = block_sum - TOK_DEV
    levels = jax.random.randint(third, (nblocks, TOK_DEV // 4), 0, 4)
    token_level = jnp.repeat(levels, 4, axis=1)
    widest = jnp.argmax(extra).astype(jnp.int32)
    chosen_token = jax.random.randint(fourth, (), 0, TOK_DEV)
    forced = (jnp.arange(nblocks, dtype=jnp.int32)[:, None] == widest) & (jnp.arange(TOK_DEV, dtype=jnp.int32)[None, :] == chosen_token)
    token_level = jnp.where(forced, 4, token_level)
    noise = jax.random.randint(fifth, (nblocks, TOK_DEV, slots), 0, 4096)
    score = (token_level[:, :, None] * 4096 + noise).reshape(nblocks, TOK_DEV * slots)
    order = jnp.argsort(-score, axis=1, stable=True)
    rank = jnp.argsort(order, axis=1, stable=True)
    taken = (rank < extra[:, None]).astype(jnp.int32)
    counts = 1 + jnp.sum(taken.reshape(nblocks, TOK_DEV, slots), axis=2)
    return counts.reshape(NTOK).astype(jnp.int32)


def shard_levels(rng, dims, shards, low, top_value):
    gain = 1.0
    for dim, parts in shards:
        draws = jax.random.uniform(jax.random.fold_in(jax.random.fold_in(rng, 6), dim), (parts,), jnp.float32, low / len(shards), top_value / len(shards))
        gain = gain * jnp.repeat(jnp.exp(draws), dims[dim] // parts).reshape((-1,) + (1,) * (len(dims) - 1 - dim))
    return gain


def gaussian(rng, extent, width, limit, cuts=(), kind=jnp.bfloat16):
    drawn = width * jax.random.normal(rng, extent, jnp.float32)
    if cuts:
        drawn = drawn * shard_levels(rng, extent, cuts, -0.22, 0.18)
    return jnp.clip(drawn, -limit, limit).astype(kind)


def setup_inputs(seed: int = 0, part: int = 0) -> dict:
    splits = jax.random.split(jax.random.key(seed), 10)
    own_keys = jax.random.split(jax.random.fold_in(splits[9], part), 10)
    return {
        "token_cond": gaussian(own_keys[0], (NTOK, CT), 1.0, 6.0, ((0, 4),)),
        "atom_feat": draw_atom_feat(jax.random.fold_in(jax.random.fold_in(splits[9], part), 71), part),
        "atom_counts": draw_atom_counts(jax.random.fold_in(jax.random.fold_in(splits[9], part), 71), part),
        "w_token": gaussian(splits[3], (CT, CA), CT ** -0.5, 0.21875),
        "w_query": gaussian(splits[4], (CA, CA), CA ** -0.5, 0.5),
        "w_key": gaussian(splits[5], (CA, CA), CA ** -0.5, 0.5),
        "w_value": gaussian(splits[6], (CA, CA), CA ** -0.5, 0.5),
        "w_out": gaussian(splits[7], (CA, CA), CA ** -0.5, 0.5),
        "w_back": gaussian(splits[8], (CA, CT), CA ** -0.5, 0.5),
    }


def reference(token_cond, atom_feat, atom_counts, w_token, w_query, w_key, w_value, w_out, w_back):
    proj = jnp.dot(token_cond, w_token, preferred_element_type=jnp.float32).astype(jnp.bfloat16)
    ends = jnp.cumsum(atom_counts).astype(jnp.int32)
    atom_ids = jnp.arange(NATOM, dtype=jnp.int32)
    owner = jnp.searchsorted(ends, atom_ids, side='right').astype(jnp.int32)
    x = (atom_feat.astype(jnp.float32) + proj[owner].astype(jnp.float32)).astype(jnp.bfloat16)
    query = jnp.dot(x, w_query, preferred_element_type=jnp.float32).astype(jnp.bfloat16)
    keyed = jnp.dot(x, w_key, preferred_element_type=jnp.float32).astype(jnp.bfloat16)
    valued = jnp.dot(x, w_value, preferred_element_type=jnp.float32).astype(jnp.bfloat16)
    blocks = NATOM // QBLOCK
    span = KEYS // QBLOCK
    padk = jnp.pad(keyed, ((HALO, HALO), (0, 0))).reshape(blocks + span - 1, QBLOCK, HEADS, HEAD)
    padv = jnp.pad(valued, ((HALO, HALO), (0, 0))).reshape(blocks + span - 1, QBLOCK, HEADS, HEAD)
    keys = jnp.concatenate([padk[j:j + blocks] for j in range(span)], axis=1)
    values = jnp.concatenate([padv[j:j + blocks] for j in range(span)], axis=1)
    qblocks = query.reshape(blocks, QBLOCK, HEADS, HEAD)
    scores = jnp.einsum('bqhd,bkhd->bhqk', qblocks.astype(jnp.float32), keys.astype(jnp.float32)) / jnp.sqrt(jnp.float32(HEAD))
    key_pos = jnp.arange(blocks, dtype=jnp.int32)[:, None] * QBLOCK + jnp.arange(KEYS, dtype=jnp.int32)[None, :] - HALO
    valid = (key_pos >= 0) & (key_pos < NATOM)
    scores = jnp.where(valid[:, None, None, :], scores, jnp.float32(-1e+30))
    weights = jax.nn.softmax(scores, axis=-1).astype(jnp.bfloat16)
    attended = jnp.einsum('bhqk,bkhd->bqhd', weights.astype(jnp.float32), values.astype(jnp.float32))
    attended = attended.reshape(NATOM, CA).astype(jnp.bfloat16)
    atom_out = (x.astype(jnp.float32) + jnp.dot(attended, w_out, preferred_element_type=jnp.float32)).astype(jnp.bfloat16)
    sums = jax.ops.segment_sum(atom_out.astype(jnp.float32), owner, num_segments=NTOK)
    pooled = (sums / atom_counts.astype(jnp.float32)[:, None]).astype(jnp.bfloat16)
    token_out = (token_cond.astype(jnp.float32) + jnp.dot(pooled, w_back, preferred_element_type=jnp.float32)).astype(jnp.bfloat16)
    return (token_out, atom_out)
```

```python
import functools
import math

import jax
import jax.numpy as jnp
from jax import lax
from jax.experimental import pallas as pl
from jax.experimental.pallas import tpu as pltpu
from jax.sharding import PartitionSpec as P

HEADS = 4
QBLOCK = 32
KEYS = 128
HALO = 48
LANES = 128
MESH = pl.DeviceIdType.MESH
F32 = jnp.float32
BF16 = jnp.bfloat16


def dot(a, b, dims=((1,), (0,))):
    return lax.dot_general(a, b, (dims, ((), ())), preferred_element_type=F32)


def greet(n, me):
    barrier = pltpu.get_barrier_semaphore()
    for d in range(1, n):
        pl.semaphore_signal(barrier, inc=1, device_id={"seq": lax.rem(me + d, n)}, device_id_type=MESH)
    pl.semaphore_wait(barrier, n - 1)


def spread(n, atom_rows, cond_ref, wtok_ref, feat_ref, counts_ref, table_ref, halo_ref, ends_ref, starts_ref,
           proj, zeros, cnt, padded, ends_all, send_sem, recv_sem, csend, crecv, lsem):
    me = lax.axis_index("seq")
    tok = cond_ref.shape[0]
    crow = tok // LANES
    right, left = lax.rem(me + 1, n), lax.rem(me + n - 1, n)
    right2, left2 = lax.rem(me + 2, n), lax.rem(me + n - 2, n)

    def remote(i, src, dst, dev):
        return pltpu.make_async_remote_copy(
            src_ref=src, dst_ref=dst, send_sem=send_sem.at[i], recv_sem=recv_sem.at[i],
            device_id={"seq": dev}, device_id_type=MESH)

    greet(n, me)
    ccopies = []
    for d in range(1, n):
        c = pltpu.make_async_remote_copy(
            src_ref=counts_ref, dst_ref=cnt.at[d - 1], send_sem=csend.at[d - 1], recv_sem=crecv.at[d - 1],
            device_id={"seq": lax.rem(me + d, n)}, device_id_type=MESH)
        c.start()
        ccopies.append(c)
    copies = [
        remote(0, feat_ref.at[pl.ds(atom_rows - HALO, HALO)], halo_ref.at[pl.ds(0, HALO)], right),
        remote(1, feat_ref.at[pl.ds(0, HALO)], halo_ref.at[pl.ds(HALO, HALO)], left),
    ]
    for c in copies:
        c.start()
    proj[...] = dot(cond_ref[...], wtok_ref[...]).astype(BF16)
    more = [
        remote(2, proj, table_ref.at[pl.ds(LANES, tok)], right),
        remote(3, proj, table_ref.at[pl.ds(LANES + 2 * tok, tok)], left),
        remote(4, proj.at[pl.ds(tok - LANES, LANES)], table_ref.at[pl.ds(0, LANES)], right2),
        remote(5, proj.at[pl.ds(0, LANES)], table_ref.at[pl.ds(LANES + 3 * tok, LANES)], left2),
    ]
    for c in more:
        c.start()
    zeros[...] = jnp.zeros_like(zeros)
    own = pltpu.make_async_copy(proj, table_ref.at[pl.ds(LANES + tok, tok)], lsem.at[0])
    own.start()
    tail = pltpu.make_async_copy(zeros, table_ref.at[pl.ds(2 * LANES + 3 * tok, LANES)], lsem.at[1])
    tail.start()

    padded[...] = jnp.zeros_like(padded)
    rows = padded.shape[0]
    for c in ccopies:
        c.wait()
    for j in range(n):
        part = jnp.where(me == j, counts_ref[...], 0)
        for d in range(1, n):
            part = jnp.where(lax.rem(me + n - d, n) == j, cnt[d - 1], part)
        padded[pl.ds(8 + crow * j, crow), :] = part
    counts = padded[...].astype(F32).astype(BF16)
    tri = (lax.broadcasted_iota(jnp.int32, (LANES, LANES), 0)
           <= lax.broadcasted_iota(jnp.int32, (LANES, LANES), 1)).astype(F32).astype(BF16)
    before = (lax.broadcasted_iota(jnp.int32, (rows, rows), 1)
              < lax.broadcasted_iota(jnp.int32, (rows, rows), 0)).astype(F32).astype(BF16)
    inner = dot(counts, tri)
    outer = jnp.sum(dot(before, counts), axis=1, keepdims=True)
    ends_all[...] = (inner + outer).astype(jnp.int32)
    near = pl.ds(8 - 1 - crow + crow * me, ends_ref.shape[0])
    ends = ends_all[near, :] - me * atom_rows
    ends_ref[...] = ends
    starts_ref[...] = ends - padded[near, :]
    for c in copies + more:
        c.wait()
    own.wait()
    tail.wait()


def atoms(n, ends_s, table, halo, feat, ends_v, starts_v, wqkv, wout, out, own, sides,
          xs, qs, ks, vs, mem, pool):
    me = lax.axis_index("seq")
    atom_rows, width = feat.shape
    tok = own.shape[0]
    head = width // HEADS
    nrow = ends_v.shape[0]
    scale = math.log2(math.e) / math.sqrt(head)
    tiles = atom_rows // LANES

    def window(first):
        w = jnp.int32(0)
        for r in range(nrow - 1):
            w += (ends_s[r, LANES - 1] <= first).astype(jnp.int32)
        return jnp.minimum(w, nrow - 3)

    def gather(first, f):
        r = f.shape[0]
        w = window(first)
        ids = first + lax.broadcasted_iota(jnp.int32, (r, LANES), 0)
        parts = []
        for s in range(2):
            lo = starts_v[pl.ds(w + s, 1), :]
            hi = ends_v[pl.ds(w + s, 1), :]
            parts.append(jnp.where((ids >= lo) & (ids < hi), F32(1), F32(0)).astype(BF16))
        member = jnp.concatenate(parts, axis=1)
        rows = dot(member, table[pl.ds(pl.multiple_of(w * LANES, LANES), 2 * LANES), :])
        x = (f.astype(F32) + rows).astype(BF16)
        return w, member, x

    def keyval(at, qkv, r):
        ks[pl.ds(at, r), :] = qkv[:, width:2 * width].astype(BF16)
        vs[pl.ds(at, r), :] = qkv[:, 2 * width:].astype(BF16)

    weights = wqkv[...]
    for first, at in ((-HALO, 0), (atom_rows, atom_rows + HALO)):
        f = halo[pl.ds(0 if first < 0 else HALO, HALO), :]
        _, _, x = gather(jnp.int32(first), f)
        keyval(at, dot(x, weights), HALO)

    def first_pass(i, c):
        for u in range(2):
            a = pl.multiple_of((2 * i + u) * LANES, LANES)
            _, member, x = gather(a, feat[pl.ds(a, LANES), :])
            mem[pl.ds(a, LANES), :] = member
            xs[pl.ds(a, LANES), :] = x
            qkv = dot(x, weights)
            qs[pl.ds(a, LANES), :] = qkv[:, :width].astype(BF16)
            keyval(pl.multiple_of(a + HALO, 16), qkv, LANES)
        return c

    lax.fori_loop(0, tiles // 2, first_pass, 0)

    pool[...] = jnp.zeros_like(pool)
    lane = lax.broadcasted_iota(jnp.int32, (1, width), 1)
    hmask = [((lane >= h * head) & (lane < (h + 1) * head)) for h in range(HEADS)]
    hmul = [jnp.where(m, F32(1), F32(0)).astype(BF16) for m in hmask]
    ones = jnp.ones((KEYS, width), BF16)
    total = atom_rows * n
    klane = lax.broadcasted_iota(jnp.int32, (1, KEYS), 1)
    per = LANES // QBLOCK
    group = 2

    def pick(o):
        r = o[(HEADS - 1) * QBLOCK:]
        for h in range(HEADS - 2, -1, -1):
            r = jnp.where(hmask[h], o[h * QBLOCK:(h + 1) * QBLOCK], r)
        return r

    def second_pass(i, c):
        base = i * group * LANES
        scores = []
        for j in range(group * per):
            at = pl.multiple_of(base + j * QBLOCK, QBLOCK)
            q = qs[pl.ds(at, QBLOCK), :]
            qb = jnp.concatenate([q * m for m in hmul], axis=0)
            s = dot(qb, ks[pl.ds(at, KEYS), :], ((1,), (1,)))
            pos = me * atom_rows + at - HALO + klane
            scores.append(jnp.where((pos >= 0) & (pos < total), s, F32(-1e30)))
        probs = []
        for s in scores:
            m = jnp.max(s, axis=1, keepdims=True)
            probs.append(jnp.exp2((s - m) * F32(scale)).astype(BF16))
        outs = []
        for j, p in enumerate(probs):
            at = pl.multiple_of(base + j * QBLOCK, QBLOCK)
            o = dot(p, jnp.concatenate([vs[pl.ds(at, KEYS), :], ones], axis=1))
            outs.append((pick(o[:, :width]) / pick(o[:, width:])).astype(BF16))
        for u in range(group):
            a = pl.multiple_of(base + u * LANES, LANES)
            att = jnp.concatenate(outs[u * per:(u + 1) * per], axis=0)
            y = (xs[pl.ds(a, LANES), :].astype(F32) + dot(att, wout[...])).astype(BF16)
            out[pl.ds(a, LANES), :] = y
            part = dot(mem[pl.ds(a, LANES), :], y, ((0,), (0,)))
            at = pl.ds(pl.multiple_of(window(a) * LANES, LANES), 2 * LANES)
            pool[at, :] += part
        return c

    lax.fori_loop(0, tiles // group, second_pass, 0)
    own[...] = pool[pl.ds(LANES + tok, tok), :]
    sides[0] = pool[pl.ds(LANES, tok), :].astype(BF16)
    sides[1] = pool[pl.ds(LANES + 2 * tok, tok), :].astype(BF16)


def merge(n, own_ref, sides_ref, counts_ref, pooled_ref, got, send_sem, recv_sem):
    me = lax.axis_index("seq")
    right, left = lax.rem(me + 1, n), lax.rem(me + n - 1, n)
    greet(n, me)
    copies = [
        pltpu.make_async_remote_copy(
            src_ref=sides_ref.at[i], dst_ref=got.at[i], send_sem=send_sem.at[i], recv_sem=recv_sem.at[i],
            device_id={"seq": dev}, device_id_type=MESH)
        for i, dev in ((0, left), (1, right))
    ]
    for c in copies:
        c.start()
    cols = [jnp.transpose(jnp.broadcast_to(counts_ref[pl.ds(r, 1), :].astype(F32), (LANES, LANES)))
            for r in range(counts_ref.shape[0])]
    for c in copies:
        c.wait()
    for r, col in enumerate(cols):
        at = pl.ds(r * LANES, LANES)
        sums = own_ref[at, :] + got[0, at, :].astype(F32) + got[1, at, :].astype(F32)
        pooled_ref[at, :] = (sums / col).astype(BF16)


VM = pl.BlockSpec(memory_space=pltpu.VMEM)
ANY = pl.BlockSpec(memory_space=pl.ANY)
SM = pl.BlockSpec(memory_space=pltpu.SMEM)


def shards(n, token_cond, atom_feat, atom_counts, w_token, w_query, w_key, w_value, w_out, w_back):
    tok, _ = token_cond.shape
    atom_rows, width = atom_feat.shape
    crow = tok // LANES
    counts = atom_counts.reshape(crow, LANES)
    nrow = 3 * crow + 4
    trows = 3 * tok + 3 * LANES
    S = jax.ShapeDtypeStruct
    DMA = pltpu.SemaphoreType.DMA
    prows = -(-(8 + crow * n + nrow) // 8) * 8
    table, halo, ends, starts = pl.pallas_call(
        functools.partial(spread, n, atom_rows),
        name="spread",
        out_shape=(S((trows, width), BF16), S((2 * HALO, width), BF16),
                   S((nrow, LANES), jnp.int32), S((nrow, LANES), jnp.int32)),
        in_specs=[VM, VM, ANY, VM],
        out_specs=(ANY, ANY, VM, VM),
        scratch_shapes=[
            pltpu.VMEM((tok, width), BF16), pltpu.VMEM((LANES, width), BF16),
            pltpu.VMEM((n - 1, crow, LANES), jnp.int32), pltpu.VMEM((prows, LANES), jnp.int32),
            pltpu.VMEM((prows, LANES), jnp.int32),
            DMA((6,)), DMA((6,)), DMA((n - 1,)), DMA((n - 1,)), DMA((2,)),
        ],
        compiler_params=pltpu.CompilerParams(collective_id=0, has_side_effects=True),
    )(token_cond, w_token, atom_feat, counts)
    wqkv = jnp.concatenate([w_query, w_key, w_value], axis=1)
    atom_out, own, sides = pl.pallas_call(
        functools.partial(atoms, n),
        name="atoms",
        out_shape=(S((atom_rows, width), BF16), S((tok, width), F32), S((2, tok, width), BF16)),
        in_specs=[SM, VM, VM, VM, VM, VM, VM, VM],
        out_specs=(VM, VM, VM),
        scratch_shapes=[
            pltpu.VMEM((atom_rows, width), BF16), pltpu.VMEM((atom_rows, width), BF16),
            pltpu.VMEM((atom_rows + 2 * HALO, width), BF16), pltpu.VMEM((atom_rows + 2 * HALO, width), BF16),
            pltpu.VMEM((atom_rows, 2 * LANES), BF16), pltpu.VMEM((trows, width), F32),
        ],
    )(ends, table, halo, atom_feat, ends, starts, wqkv, w_out)
    pooled = pl.pallas_call(
        functools.partial(merge, n),
        name="merge",
        out_shape=S((tok, width), BF16),
        in_specs=[VM, VM, VM],
        out_specs=VM,
        scratch_shapes=[pltpu.VMEM((2, tok, width), BF16), DMA((2,)), DMA((2,))],
        compiler_params=pltpu.CompilerParams(collective_id=1, has_side_effects=True),
    )(own, sides, counts)
    token_out = (
        token_cond.astype(F32) + jnp.dot(pooled, w_back, preferred_element_type=F32)
    ).astype(BF16)
    return (token_out, atom_out)


def solution(mesh):
    both = P(("batch", "seq"), None)
    in_specs = (both, both, P(("batch", "seq")), P(), P(), P(), P(), P(), P())
    return jax.shard_map(
        functools.partial(shards, mesh.shape["seq"]), mesh=mesh, in_specs=in_specs, out_specs=(both, both),
        check_vma=False)
```

```python
import functools
import math

import jax
import jax.numpy as jnp
from jax import lax
from jax.experimental import pallas as pl
from jax.experimental.pallas import tpu as pltpu
from jax.sharding import PartitionSpec as P

HEADS = 4
QBLOCK = 32
KEYS = 128
HALO = 48
LANES = 128
MESH = pl.DeviceIdType.MESH
F32 = jnp.float32
BF16 = jnp.bfloat16


def dot(a, b, dims=((1,), (0,))):
    return lax.dot_general(a, b, (dims, ((), ())), preferred_element_type=F32)


def greet(n, me):
    barrier = pltpu.get_barrier_semaphore()
    for d in range(1, n):
        pl.semaphore_signal(barrier, inc=1, device_id={"seq": lax.rem(me + d, n)}, device_id_type=MESH)
    return lambda: pl.semaphore_wait(barrier, n - 1)


def spread(n, atom_rows, cond_ref, wtok_ref, feat_ref, counts_ref, table_ref, halo_ref, ends_ref, starts_ref, wins_ref,
           proj, zeros, cnt, padded, ends_all, send_sem, recv_sem, csend, crecv, lsem):
    me = lax.axis_index("seq")
    tok = cond_ref.shape[0]
    crow = tok // LANES
    right, left = lax.rem(me + 1, n), lax.rem(me + n - 1, n)
    right2, left2 = lax.rem(me + 2, n), lax.rem(me + n - 2, n)

    def remote(i, src, dst, dev):
        return pltpu.make_async_remote_copy(
            src_ref=src, dst_ref=dst, send_sem=send_sem.at[i], recv_sem=recv_sem.at[i],
            device_id={"seq": dev}, device_id_type=MESH)

    arrive = greet(n, me)
    half = tok // 2
    proj[pl.ds(0, half), :] = dot(cond_ref[pl.ds(0, half), :], wtok_ref[...]).astype(BF16)
    arrive()
    ccopies = []
    for d in range(1, n):
        c = pltpu.make_async_remote_copy(
            src_ref=counts_ref, dst_ref=cnt.at[d - 1], send_sem=csend.at[d - 1], recv_sem=crecv.at[d - 1],
            device_id={"seq": lax.rem(me + d, n)}, device_id_type=MESH)
        c.start()
        ccopies.append(c)

    def pair(i, at):
        return [
            remote(i, proj.at[pl.ds(at, half)], table_ref.at[pl.ds(LANES + at, half)], right),
            remote(i + 1, proj.at[pl.ds(at, half)], table_ref.at[pl.ds(LANES + 2 * tok + at, half)], left),
        ]

    copies = pair(0, 0)
    for c in copies:
        c.start()
    proj[pl.ds(half, half), :] = dot(cond_ref[pl.ds(half, half), :], wtok_ref[...]).astype(BF16)
    more = pair(2, half) + [
        remote(4, proj.at[pl.ds(tok - LANES, LANES)], table_ref.at[pl.ds(0, LANES)], right2),
        remote(5, proj.at[pl.ds(0, LANES)], table_ref.at[pl.ds(LANES + 3 * tok, LANES)], left2),
        remote(6, feat_ref.at[pl.ds(atom_rows - HALO, HALO)], halo_ref.at[pl.ds(0, HALO)], right),
        remote(7, feat_ref.at[pl.ds(0, HALO)], halo_ref.at[pl.ds(HALO, HALO)], left),
    ]
    for c in more:
        c.start()
    zeros[...] = jnp.zeros_like(zeros)
    own = pltpu.make_async_copy(proj, table_ref.at[pl.ds(LANES + tok, tok)], lsem.at[0])
    own.start()
    tail = pltpu.make_async_copy(zeros, table_ref.at[pl.ds(2 * LANES + 3 * tok, LANES)], lsem.at[1])
    tail.start()

    padded[...] = jnp.zeros_like(padded)
    rows = padded.shape[0]
    for c in ccopies:
        c.wait()
    for j in range(n):
        part = jnp.where(me == j, counts_ref[...], 0)
        for d in range(1, n):
            part = jnp.where(lax.rem(me + n - d, n) == j, cnt[d - 1], part)
        padded[pl.ds(8 + crow * j, crow), :] = part
    counts = padded[...].astype(F32).astype(BF16)
    tri = (lax.broadcasted_iota(jnp.int32, (LANES, LANES), 0)
           <= lax.broadcasted_iota(jnp.int32, (LANES, LANES), 1)).astype(F32).astype(BF16)
    before = (lax.broadcasted_iota(jnp.int32, (rows, rows), 1)
              < lax.broadcasted_iota(jnp.int32, (rows, rows), 0)).astype(F32).astype(BF16)
    inner = dot(counts, tri)
    outer = jnp.sum(dot(before, counts), axis=1, keepdims=True)
    ends_all[...] = (inner + outer).astype(jnp.int32)
    near = pl.ds(8 - 1 - crow + crow * me, ends_ref.shape[0])
    ends = ends_all[near, :] - me * atom_rows
    ends_ref[...] = ends
    starts_ref[...] = ends - padded[near, :]
    first = jnp.where(lax.broadcasted_iota(jnp.int32, wins_ref.shape, 0) == 0,
                      lax.broadcasted_iota(jnp.int32, wins_ref.shape, 1) * LANES, -HALO)
    w = jnp.zeros_like(first)
    for r in range(ends_ref.shape[0] - 1):
        w += jnp.where(ends[r:r + 1, LANES - 1:] <= first, 1, 0)
    wins_ref[...] = jnp.minimum(w, ends_ref.shape[0] - 3)
    for c in copies + more:
        c.wait()
    own.wait()
    tail.wait()


def atoms(n, group, wins, table, halo, feat, ends_v, starts_v, wq, wk, wv, wout, out, own, sides,
          obuf, wqkv, xs, qs, ks, vs, att, mem, pool, osem):
    me = lax.axis_index("seq")
    atom_rows, width = feat.shape
    tok = own.shape[0]
    head = width // HEADS
    nrow = ends_v.shape[0]
    scale = math.log2(math.e) / math.sqrt(head)
    step = group * LANES
    tiles = atom_rows // LANES
    groups = atom_rows // step
    spare = pool.shape[0] - 2 * LANES

    def store(g):
        at = pl.ds(pl.multiple_of(g * step, step), step)
        return pltpu.make_async_copy(obuf.at[at], out.at[at], osem.at[g])

    def each(f):
        def body(g, c):
            f(g)
            return c
        return body

    for i, w in enumerate((wq, wk, wv)):
        wqkv[:, i * width:(i + 1) * width] = w[...]

    def gather(w, first, f):
        r = f.shape[0]
        ids = first + lax.broadcasted_iota(jnp.int32, (r, LANES), 0)
        parts = []
        for s in range(2):
            lo = starts_v[pl.ds(w + s, 1), :]
            hi = ends_v[pl.ds(w + s, 1), :]
            parts.append(jnp.where((ids >= lo) & (ids < hi), F32(1), F32(0)).astype(BF16))
        member = jnp.concatenate(parts, axis=1)
        rows = dot(member, table[pl.ds(pl.multiple_of(w * LANES, LANES), 2 * LANES), :])
        x = (f.astype(F32) + rows).astype(BF16)
        return member, x

    def keyval(at, qkv, r):
        ks[pl.ds(at, r), :] = qkv[:, width:2 * width].astype(BF16)
        vs[pl.ds(at, r), :] = qkv[:, 2 * width:].astype(BF16)

    for first, at in ((-HALO, 0), (atom_rows, atom_rows + HALO)):
        f = halo[pl.ds(0 if first < 0 else HALO, HALO), :]
        w = wins[1, 0] if first < 0 else wins[0, tiles]
        _, x = gather(w, jnp.int32(first), f)
        keyval(at, dot(x, wqkv[...]), HALO)
    pool[...] = jnp.zeros_like(pool)

    lane = lax.broadcasted_iota(jnp.int32, (1, width), 1)
    hmask = [((lane >= h * head) & (lane < (h + 1) * head)) for h in range(HEADS)]
    hmul = [jnp.where(m, F32(1), F32(0)).astype(BF16) for m in hmask]
    ones = jnp.ones((KEYS, width), BF16)
    total = atom_rows * n
    klane = lax.broadcasted_iota(jnp.int32, (1, KEYS), 1)
    per = LANES // QBLOCK

    def pick(o):
        r = o[(HEADS - 1) * QBLOCK:]
        for h in range(HEADS - 2, -1, -1):
            r = jnp.where(hmask[h], o[h * QBLOCK:(h + 1) * QBLOCK], r)
        return r

    def gathers(g):
        made = []
        for u in range(group):
            a = pl.multiple_of(g * step + u * LANES, LANES)
            made.append((a, *gather(wins[0, g * group + u], a, feat[pl.ds(a, LANES), :])))
        return made

    def project(g, made):
        qkvs = [dot(x, wqkv[...]) for _, _, x in made]
        for (a, member, x), qkv in zip(made, qkvs):
            mem[pl.ds(a, LANES), :] = member
            xs[pl.ds(a, LANES), :] = x
            qs[pl.ds(a, LANES), :] = qkv[:, :width].astype(BF16)
            keyval(pl.multiple_of(a + HALO, 16), qkv, LANES)

    def scored(g, js):
        scores = []
        for j in js:
            at = pl.multiple_of(g * step + j * QBLOCK, QBLOCK)
            q = qs[pl.ds(at, QBLOCK), :]
            qb = jnp.concatenate([q * m for m in hmul], axis=0)
            s = dot(qb, ks[pl.ds(at, KEYS), :], ((1,), (1,)))
            pos = me * atom_rows + at - HALO + klane
            scores.append(jnp.where((pos >= 0) & (pos < total), s, F32(-1e30)))
        return scores

    def soft(scores):
        probs = []
        for s in scores:
            m = jnp.max(s, axis=1, keepdims=True)
            probs.append(jnp.exp2((s - m) * F32(scale)).astype(BF16))
        return probs

    def attend(g, js, probs):
        raw = []
        for j, p in zip(js, probs):
            at = pl.multiple_of(g * step + j * QBLOCK, QBLOCK)
            raw.append(dot(p, jnp.concatenate([vs[pl.ds(at, KEYS), :], ones], axis=1)))
        return [(pick(o[:, :width]) / pick(o[:, width:])).astype(BF16) for o in raw]

    def residual(g):
        at = pl.ds(pl.multiple_of(g * step, step), step)
        y = (xs[at, :].astype(F32) + dot(att[at, :], wout[...])).astype(BF16)
        obuf[at, :] = y
        return y

    def pooled(g, y, real):
        parts = [dot(mem[pl.ds(pl.multiple_of(g * step + u * LANES, LANES), LANES), :],
                     y[u * LANES:(u + 1) * LANES], ((0,), (0,))) for u in range(group)]
        for u, part in enumerate(parts):
            first = jnp.where(real, wins[0, g * group + u] * LANES, spare)
            pool[pl.ds(pl.multiple_of(first, LANES), 2 * LANES), :] += part

    early, late = range(group * per // 2), range(group * per // 2, group * per)
    ahead = 2

    def advance(g, more):
        past = jnp.maximum(g - 1, 0)
        s0 = scored(g, early)
        y = residual(past)
        made = gathers(g + ahead) if more else None
        p0 = soft(s0)
        s1 = scored(g, late)
        pooled(past, y, g > 0)
        o0 = attend(g, early, p0)
        p1 = soft(s1)
        o1 = attend(g, late, p1)
        if more:
            project(g + ahead, made)
        att[pl.ds(pl.multiple_of(g * step, step), step), :] = jnp.concatenate(o0 + o1, axis=0)

        @pl.when(g > 0)
        def _():
            store(past).start()

    lax.fori_loop(0, ahead, each(lambda g: project(g, gathers(g))), 0)
    lax.fori_loop(0, groups - ahead, each(lambda g: advance(g, True)), 0)
    lax.fori_loop(groups - ahead, groups, each(lambda g: advance(g, False)), 0)
    y = residual(groups - 1)
    store(groups - 1).start()
    pooled(groups - 1, y, True)
    own[...] = pool[pl.ds(LANES + tok, tok), :]
    sides[0] = pool[pl.ds(LANES, tok), :].astype(BF16)
    sides[1] = pool[pl.ds(LANES + 2 * tok, tok), :].astype(BF16)
    lax.fori_loop(0, groups, each(lambda g: store(g).wait()), 0)


def merge(n, own_ref, sides_ref, counts_ref, pooled_ref, got, send_sem, recv_sem):
    me = lax.axis_index("seq")
    right, left = lax.rem(me + 1, n), lax.rem(me + n - 1, n)
    greet(n, me)()
    copies = [
        pltpu.make_async_remote_copy(
            src_ref=sides_ref.at[i], dst_ref=got.at[i], send_sem=send_sem.at[i], recv_sem=recv_sem.at[i],
            device_id={"seq": dev}, device_id_type=MESH)
        for i, dev in ((0, left), (1, right))
    ]
    for c in copies:
        c.start()
    cols = [jnp.transpose(jnp.broadcast_to(counts_ref[pl.ds(r, 1), :].astype(F32), (LANES, LANES)))
            for r in range(counts_ref.shape[0])]
    for c in copies:
        c.wait()
    for r, col in enumerate(cols):
        at = pl.ds(r * LANES, LANES)
        sums = own_ref[at, :] + got[0, at, :].astype(F32) + got[1, at, :].astype(F32)
        pooled_ref[at, :] = (sums / col).astype(BF16)


VM = pl.BlockSpec(memory_space=pltpu.VMEM)
ANY = pl.BlockSpec(memory_space=pl.ANY)
HBM = pl.BlockSpec(memory_space=pltpu.HBM)
SM = pl.BlockSpec(memory_space=pltpu.SMEM)


def shards(n, token_cond, atom_feat, atom_counts, w_token, w_query, w_key, w_value, w_out, w_back):
    tok, _ = token_cond.shape
    atom_rows, width = atom_feat.shape
    crow = tok // LANES
    counts = atom_counts.reshape(crow, LANES)
    nrow = 3 * crow + 4
    trows = 3 * tok + 3 * LANES
    S = jax.ShapeDtypeStruct
    DMA = pltpu.SemaphoreType.DMA
    prows = -(-(8 + crow * n + nrow) // 8) * 8
    table, halo, ends, starts, wins = pl.pallas_call(
        functools.partial(spread, n, atom_rows),
        name="spread",
        out_shape=(S((trows, width), BF16), S((2 * HALO, width), BF16),
                   S((nrow, LANES), jnp.int32), S((nrow, LANES), jnp.int32),
                   S((8, LANES), jnp.int32)),
        in_specs=[VM, VM, HBM, VM],
        out_specs=(ANY, ANY, VM, VM, VM),
        scratch_shapes=[
            pltpu.VMEM((tok, width), BF16), pltpu.VMEM((LANES, width), BF16),
            pltpu.VMEM((n - 1, crow, LANES), jnp.int32), pltpu.VMEM((prows, LANES), jnp.int32),
            pltpu.VMEM((prows, LANES), jnp.int32),
            DMA((8,)), DMA((8,)), DMA((n - 1,)), DMA((n - 1,)), DMA((2,)),
        ],
        compiler_params=pltpu.CompilerParams(collective_id=0, has_side_effects=True, vmem_limit_bytes=8 << 20),
    )(token_cond, w_token, atom_feat, counts)
    group = 2
    groups = atom_rows // (group * LANES)
    atom_out, own, sides = pl.pallas_call(
        functools.partial(atoms, n, group),
        name="atoms",
        out_shape=(S((atom_rows, width), BF16), S((tok, width), F32), S((2, tok, width), BF16)),
        in_specs=[SM, VM, VM, VM, VM, VM, VM, VM, VM, VM],
        out_specs=(ANY, VM, VM),
        scratch_shapes=[
            pltpu.VMEM((atom_rows, width), BF16), pltpu.VMEM((width, 3 * width), BF16),
            pltpu.VMEM((atom_rows, width), BF16), pltpu.VMEM((atom_rows, width), BF16),
            pltpu.VMEM((atom_rows + 2 * HALO, width), BF16), pltpu.VMEM((atom_rows + 2 * HALO, width), BF16),
            pltpu.VMEM((atom_rows, width), BF16), pltpu.VMEM((atom_rows, 2 * LANES), BF16),
            pltpu.VMEM((trows + 2 * LANES, width), F32),
            DMA((groups,)),
        ],
        compiler_params=pltpu.CompilerParams(vmem_limit_bytes=24 << 20),
    )(wins, table, halo, atom_feat, ends, starts, w_query, w_key, w_value, w_out)
    pooled = pl.pallas_call(
        functools.partial(merge, n),
        name="merge",
        out_shape=S((tok, width), BF16),
        in_specs=[VM, VM, VM],
        out_specs=VM,
        scratch_shapes=[pltpu.VMEM((2, tok, width), BF16), DMA((2,)), DMA((2,))],
        compiler_params=pltpu.CompilerParams(collective_id=1, has_side_effects=True, vmem_limit_bytes=8 << 20),
    )(own, sides, counts)
    token_out = (
        token_cond.astype(F32) + jnp.dot(pooled, w_back, preferred_element_type=F32)
    ).astype(BF16)
    return (token_out, atom_out)


def solution(mesh):
    both = P(("batch", "seq"), None)
    in_specs = (both, both, P(("batch", "seq")), P(), P(), P(), P(), P(), P())
    return jax.shard_map(
        functools.partial(shards, mesh.shape["seq"]), mesh=mesh, in_specs=in_specs, out_specs=(both, both),
        check_vma=False)
```

```python
import functools
import math

import jax
import jax.numpy as jnp
from jax import lax
from jax.experimental import pallas as pl
from jax.experimental.pallas import tpu as pltpu
from jax.sharding import PartitionSpec as P

HEADS = 4
QBLOCK = 32
KEYS = 128
HALO = 48
LANES = 128
MESH = pl.DeviceIdType.MESH
F32 = jnp.float32
BF16 = jnp.bfloat16


def dot(a, b, dims=((1,), (0,))):
    return lax.dot_general(a, b, (dims, ((), ())), preferred_element_type=F32)


def greet(n, me):
    barrier = pltpu.get_barrier_semaphore()
    for d in range(1, n):
        pl.semaphore_signal(barrier, inc=1, device_id={"seq": lax.rem(me + d, n)}, device_id_type=MESH)
    return lambda: pl.semaphore_wait(barrier, n - 1)


def spread(n, atom_rows, cond_hbm, wtok_hbm, feat_ref, counts_ref, table_ref, halo_ref, ends_ref, starts_ref, wins_ref,
           cond_ref, wtok_ref, proj, zeros, cnt, padded, ends_all, send_sem, recv_sem, csend, crecv, lsem):
    me = lax.axis_index("seq")
    tok = cond_ref.shape[0]
    crow = tok // LANES
    right, left = lax.rem(me + 1, n), lax.rem(me + n - 1, n)
    right2, left2 = lax.rem(me + 2, n), lax.rem(me + n - 2, n)

    def remote(i, src, dst, dev):
        return pltpu.make_async_remote_copy(
            src_ref=src, dst_ref=dst, send_sem=send_sem.at[i], recv_sem=recv_sem.at[i],
            device_id={"seq": dev}, device_id_type=MESH)

    half = tok // 2
    loads = [pltpu.make_async_copy(wtok_hbm, wtok_ref, lsem.at[2])] + [
        pltpu.make_async_copy(cond_hbm.at[pl.ds(i * half, half)], cond_ref.at[pl.ds(i * half, half)], lsem.at[3 + i])
        for i in range(2)]
    for c in loads:
        c.start()
    arrive = greet(n, me)
    loads[0].wait()
    loads[1].wait()
    proj[pl.ds(0, half), :] = dot(cond_ref[pl.ds(0, half), :], wtok_ref[...]).astype(BF16)
    arrive()
    ccopies = []
    for d in range(1, n):
        c = pltpu.make_async_remote_copy(
            src_ref=counts_ref, dst_ref=cnt.at[d - 1], send_sem=csend.at[d - 1], recv_sem=crecv.at[d - 1],
            device_id={"seq": lax.rem(me + d, n)}, device_id_type=MESH)
        c.start()
        ccopies.append(c)

    def pair(i, at):
        return [
            remote(i, proj.at[pl.ds(at, half)], table_ref.at[pl.ds(LANES + at, half)], right),
            remote(i + 1, proj.at[pl.ds(at, half)], table_ref.at[pl.ds(LANES + 2 * tok + at, half)], left),
        ]

    copies = pair(0, 0)
    for c in copies:
        c.start()
    loads[2].wait()
    proj[pl.ds(half, half), :] = dot(cond_ref[pl.ds(half, half), :], wtok_ref[...]).astype(BF16)
    more = pair(2, half) + [
        remote(4, proj.at[pl.ds(tok - LANES, LANES)], table_ref.at[pl.ds(0, LANES)], right2),
        remote(5, proj.at[pl.ds(0, LANES)], table_ref.at[pl.ds(LANES + 3 * tok, LANES)], left2),
        remote(6, feat_ref.at[pl.ds(atom_rows - HALO, HALO)], halo_ref.at[pl.ds(0, HALO)], right),
        remote(7, feat_ref.at[pl.ds(0, HALO)], halo_ref.at[pl.ds(HALO, HALO)], left),
    ]
    for c in more:
        c.start()
    zeros[...] = jnp.zeros_like(zeros)
    own = pltpu.make_async_copy(proj, table_ref.at[pl.ds(LANES + tok, tok)], lsem.at[0])
    own.start()
    tail = pltpu.make_async_copy(zeros, table_ref.at[pl.ds(2 * LANES + 3 * tok, LANES)], lsem.at[1])
    tail.start()

    padded[...] = jnp.zeros_like(padded)
    rows = padded.shape[0]
    for c in ccopies:
        c.wait()
    for j in range(n):
        part = jnp.where(me == j, counts_ref[...], 0)
        for d in range(1, n):
            part = jnp.where(lax.rem(me + n - d, n) == j, cnt[d - 1], part)
        padded[pl.ds(8 + crow * j, crow), :] = part
    counts = padded[...].astype(F32).astype(BF16)
    tri = (lax.broadcasted_iota(jnp.int32, (LANES, LANES), 0)
           <= lax.broadcasted_iota(jnp.int32, (LANES, LANES), 1)).astype(F32).astype(BF16)
    before = (lax.broadcasted_iota(jnp.int32, (rows, rows), 1)
              < lax.broadcasted_iota(jnp.int32, (rows, rows), 0)).astype(F32).astype(BF16)
    inner = dot(counts, tri)
    outer = jnp.sum(dot(before, counts), axis=1, keepdims=True)
    ends_all[...] = (inner + outer).astype(jnp.int32)
    near = pl.ds(8 - 1 - crow + crow * me, ends_ref.shape[0])
    ends = ends_all[near, :] - me * atom_rows
    ends_ref[...] = ends
    starts_ref[...] = ends - padded[near, :]
    first = jnp.where(lax.broadcasted_iota(jnp.int32, wins_ref.shape, 0) == 0,
                      lax.broadcasted_iota(jnp.int32, wins_ref.shape, 1) * LANES, -HALO)
    w = jnp.zeros_like(first)
    for r in range(ends_ref.shape[0] - 1):
        w += jnp.where(ends[r:r + 1, LANES - 1:] <= first, 1, 0)
    wins_ref[...] = jnp.minimum(w, ends_ref.shape[0] - 3)
    for c in copies + more:
        c.wait()
    own.wait()
    tail.wait()


def atoms(n, group, wins, table, halo, feat_hbm, ends_v, starts_v, wq, wk, wv, wout, out, own, sides,
          feat, obuf, wqkv, xs, qs, ks, vs, att, mem, pool, fsem, osem):
    me = lax.axis_index("seq")
    atom_rows, width = feat.shape
    tok = own.shape[0]
    head = width // HEADS
    nrow = ends_v.shape[0]
    scale = math.log2(math.e) / math.sqrt(head)
    step = group * LANES
    tiles = atom_rows // LANES
    groups = atom_rows // step
    spare = pool.shape[0] - 2 * LANES

    def load(g):
        at = pl.ds(pl.multiple_of(g * step, step), step)
        return pltpu.make_async_copy(feat_hbm.at[at], feat.at[at], fsem.at[g])

    def store(g):
        at = pl.ds(pl.multiple_of(g * step, step), step)
        return pltpu.make_async_copy(obuf.at[at], out.at[at], osem.at[g])

    def each(f):
        def body(g, c):
            f(g)
            return c
        return body

    lax.fori_loop(0, groups, each(lambda g: load(g).start()), 0)
    for i, w in enumerate((wq, wk, wv)):
        wqkv[:, i * width:(i + 1) * width] = w[...]

    def gather(w, first, f):
        r = f.shape[0]
        ids = first + lax.broadcasted_iota(jnp.int32, (r, LANES), 0)
        parts = []
        for s in range(2):
            lo = starts_v[pl.ds(w + s, 1), :]
            hi = ends_v[pl.ds(w + s, 1), :]
            parts.append(jnp.where((ids >= lo) & (ids < hi), F32(1), F32(0)).astype(BF16))
        member = jnp.concatenate(parts, axis=1)
        rows = dot(member, table[pl.ds(pl.multiple_of(w * LANES, LANES), 2 * LANES), :])
        x = (f.astype(F32) + rows).astype(BF16)
        return member, x

    def keyval(at, qkv, r):
        ks[pl.ds(at, r), :] = qkv[:, width:2 * width].astype(BF16)
        vs[pl.ds(at, r), :] = qkv[:, 2 * width:].astype(BF16)

    for first, at in ((-HALO, 0), (atom_rows, atom_rows + HALO)):
        f = halo[pl.ds(0 if first < 0 else HALO, HALO), :]
        w = wins[1, 0] if first < 0 else wins[0, tiles]
        _, x = gather(w, jnp.int32(first), f)
        keyval(at, dot(x, wqkv[...]), HALO)
    pool[...] = jnp.zeros_like(pool)

    lane = lax.broadcasted_iota(jnp.int32, (1, width), 1)
    hmask = [((lane >= h * head) & (lane < (h + 1) * head)) for h in range(HEADS)]
    hmul = [jnp.where(m, F32(1), F32(0)).astype(BF16) for m in hmask]
    ones = jnp.ones((KEYS, width), BF16)
    total = atom_rows * n
    klane = lax.broadcasted_iota(jnp.int32, (1, KEYS), 1)
    per = LANES // QBLOCK

    def pick(o):
        r = o[(HEADS - 1) * QBLOCK:]
        for h in range(HEADS - 2, -1, -1):
            r = jnp.where(hmask[h], o[h * QBLOCK:(h + 1) * QBLOCK], r)
        return r

    def gathers(g):
        made = []
        for u in range(group):
            a = pl.multiple_of(g * step + u * LANES, LANES)
            made.append((a, *gather(wins[0, g * group + u], a, feat[pl.ds(a, LANES), :])))
        return made

    def project(g, made):
        qkvs = [dot(x, wqkv[...]) for _, _, x in made]
        for (a, member, x), qkv in zip(made, qkvs):
            mem[pl.ds(a, LANES), :] = member
            xs[pl.ds(a, LANES), :] = x
            qs[pl.ds(a, LANES), :] = qkv[:, :width].astype(BF16)
            keyval(pl.multiple_of(a + HALO, 16), qkv, LANES)

    def scored(g, js):
        scores = []
        for j in js:
            at = pl.multiple_of(g * step + j * QBLOCK, QBLOCK)
            q = qs[pl.ds(at, QBLOCK), :]
            qb = jnp.concatenate([q * m for m in hmul], axis=0)
            s = dot(qb, ks[pl.ds(at, KEYS), :], ((1,), (1,)))
            pos = me * atom_rows + at - HALO + klane
            scores.append(jnp.where((pos >= 0) & (pos < total), s, F32(-1e30)))
        return scores

    def soft(scores):
        probs = []
        for s in scores:
            m = jnp.max(s, axis=1, keepdims=True)
            probs.append(jnp.exp2((s - m) * F32(scale)).astype(BF16))
        return probs

    def attend(g, js, probs):
        raw = []
        for j, p in zip(js, probs):
            at = pl.multiple_of(g * step + j * QBLOCK, QBLOCK)
            raw.append(dot(p, jnp.concatenate([vs[pl.ds(at, KEYS), :], ones], axis=1)))
        return [(pick(o[:, :width]) / pick(o[:, width:])).astype(BF16) for o in raw]

    def residual(g):
        at = pl.ds(pl.multiple_of(g * step, step), step)
        y = (xs[at, :].astype(F32) + dot(att[at, :], wout[...])).astype(BF16)
        obuf[at, :] = y
        return y

    def pooled(g, y, real):
        parts = [dot(mem[pl.ds(pl.multiple_of(g * step + u * LANES, LANES), LANES), :],
                     y[u * LANES:(u + 1) * LANES], ((0,), (0,))) for u in range(group)]
        for u, part in enumerate(parts):
            first = jnp.where(real, wins[0, g * group + u] * LANES, spare)
            pool[pl.ds(pl.multiple_of(first, LANES), 2 * LANES), :] += part

    early, late = range(group * per // 2), range(group * per // 2, group * per)
    ahead = 2

    def advance(g, more):
        past = jnp.maximum(g - 1, 0)
        if more:
            load(g + ahead).wait()
        s0 = scored(g, early)
        y = residual(past)
        made = gathers(g + ahead) if more else None
        p0 = soft(s0)
        s1 = scored(g, late)
        pooled(past, y, g > 0)
        o0 = attend(g, early, p0)
        p1 = soft(s1)
        o1 = attend(g, late, p1)
        if more:
            project(g + ahead, made)
        att[pl.ds(pl.multiple_of(g * step, step), step), :] = jnp.concatenate(o0 + o1, axis=0)

        @pl.when(g > 0)
        def _():
            store(past).start()

    def begin(g):
        load(g).wait()
        project(g, gathers(g))

    lax.fori_loop(0, ahead, each(begin), 0)
    lax.fori_loop(0, groups - ahead, each(lambda g: advance(g, True)), 0)
    lax.fori_loop(groups - ahead, groups, each(lambda g: advance(g, False)), 0)
    y = residual(groups - 1)
    store(groups - 1).start()
    pooled(groups - 1, y, True)
    own[...] = pool[pl.ds(LANES + tok, tok), :]
    sides[0] = pool[pl.ds(LANES, tok), :].astype(BF16)
    sides[1] = pool[pl.ds(LANES + 2 * tok, tok), :].astype(BF16)
    lax.fori_loop(0, groups, each(lambda g: store(g).wait()), 0)


def merge(n, own_ref, sides_ref, counts_ref, pooled_ref, got, send_sem, recv_sem):
    me = lax.axis_index("seq")
    right, left = lax.rem(me + 1, n), lax.rem(me + n - 1, n)
    greet(n, me)()
    copies = [
        pltpu.make_async_remote_copy(
            src_ref=sides_ref.at[i], dst_ref=got.at[i], send_sem=send_sem.at[i], recv_sem=recv_sem.at[i],
            device_id={"seq": dev}, device_id_type=MESH)
        for i, dev in ((0, left), (1, right))
    ]
    for c in copies:
        c.start()
    cols = [jnp.transpose(jnp.broadcast_to(counts_ref[pl.ds(r, 1), :].astype(F32), (LANES, LANES)))
            for r in range(counts_ref.shape[0])]
    for c in copies:
        c.wait()
    for r, col in enumerate(cols):
        at = pl.ds(r * LANES, LANES)
        sums = own_ref[at, :] + got[0, at, :].astype(F32) + got[1, at, :].astype(F32)
        pooled_ref[at, :] = (sums / col).astype(BF16)


VM = pl.BlockSpec(memory_space=pltpu.VMEM)
ANY = pl.BlockSpec(memory_space=pl.ANY)
HBM = pl.BlockSpec(memory_space=pltpu.HBM)
SM = pl.BlockSpec(memory_space=pltpu.SMEM)


def shards(n, token_cond, atom_feat, atom_counts, w_token, w_query, w_key, w_value, w_out, w_back):
    tok, _ = token_cond.shape
    atom_rows, width = atom_feat.shape
    crow = tok // LANES
    counts = atom_counts.reshape(crow, LANES)
    nrow = 3 * crow + 4
    trows = 3 * tok + 3 * LANES
    S = jax.ShapeDtypeStruct
    DMA = pltpu.SemaphoreType.DMA
    prows = -(-(8 + crow * n + nrow) // 8) * 8
    table, halo, ends, starts, wins = pl.pallas_call(
        functools.partial(spread, n, atom_rows),
        name="spread",
        out_shape=(S((trows, width), BF16), S((2 * HALO, width), BF16),
                   S((nrow, LANES), jnp.int32), S((nrow, LANES), jnp.int32),
                   S((8, LANES), jnp.int32)),
        in_specs=[HBM, HBM, HBM, VM],
        out_specs=(ANY, ANY, VM, VM, VM),
        scratch_shapes=[
            pltpu.VMEM(token_cond.shape, BF16), pltpu.VMEM(w_token.shape, BF16),
            pltpu.VMEM((tok, width), BF16), pltpu.VMEM((LANES, width), BF16),
            pltpu.VMEM((n - 1, crow, LANES), jnp.int32), pltpu.VMEM((prows, LANES), jnp.int32),
            pltpu.VMEM((prows, LANES), jnp.int32),
            DMA((8,)), DMA((8,)), DMA((n - 1,)), DMA((n - 1,)), DMA((5,)),
        ],
        compiler_params=pltpu.CompilerParams(collective_id=0, has_side_effects=True, vmem_limit_bytes=62 << 20),
    )(token_cond, w_token, atom_feat, counts)
    group = 2
    groups = atom_rows // (group * LANES)
    atom_out, own, sides = pl.pallas_call(
        functools.partial(atoms, n, group),
        name="atoms",
        out_shape=(S((atom_rows, width), BF16), S((tok, width), F32), S((2, tok, width), BF16)),
        in_specs=[SM, VM, VM, HBM, VM, VM, VM, VM, VM, VM],
        out_specs=(ANY, VM, VM),
        scratch_shapes=[
            pltpu.VMEM((atom_rows, width), BF16),
            pltpu.VMEM((atom_rows, width), BF16), pltpu.VMEM((width, 3 * width), BF16),
            pltpu.VMEM((atom_rows, width), BF16), pltpu.VMEM((atom_rows, width), BF16),
            pltpu.VMEM((atom_rows + 2 * HALO, width), BF16), pltpu.VMEM((atom_rows + 2 * HALO, width), BF16),
            pltpu.VMEM((atom_rows, width), BF16), pltpu.VMEM((atom_rows, 2 * LANES), BF16),
            pltpu.VMEM((trows + 2 * LANES, width), F32),
            DMA((groups,)), DMA((groups,)),
        ],
        compiler_params=pltpu.CompilerParams(vmem_limit_bytes=62 << 20),
    )(wins, table, halo, atom_feat, ends, starts, w_query, w_key, w_value, w_out)
    pooled = pl.pallas_call(
        functools.partial(merge, n),
        name="merge",
        out_shape=S((tok, width), BF16),
        in_specs=[VM, VM, VM],
        out_specs=VM,
        scratch_shapes=[pltpu.VMEM((2, tok, width), BF16), DMA((2,)), DMA((2,))],
        compiler_params=pltpu.CompilerParams(collective_id=1, has_side_effects=True, vmem_limit_bytes=62 << 20),
    )(own, sides, counts)
    token_out = (
        token_cond.astype(F32) + jnp.dot(pooled, w_back, preferred_element_type=F32)
    ).astype(BF16)
    return (token_out, atom_out)


def solution(mesh):
    both = P(("batch", "seq"), None)
    in_specs = (both, both, P(("batch", "seq")), P(), P(), P(), P(), P(), P())
    return jax.shard_map(
        functools.partial(shards, mesh.shape["seq"]), mesh=mesh, in_specs=in_specs, out_specs=(both, both),
        check_vma=False)
```
